128 devices in a mesh: pole: 8 (over x, z_lo), blk: 16 (over y, z_hi, core).
Axes of the slice: x: 4, y: 4, z: 4 (z_hi: 2, z_lo: 2; z = z_hi * 2 + z_lo), core: 2. Of those that a mesh axis runs over, the one named last changes fastest.
Arguments:
- inverse_block: float32 [8, 2, 4096, 4096], P('pole', None, 'blk'), may hold values from -0.09375 to 0.09375
- factor: float32 [8, 4096, 2, 512], P('pole', 'blk'), may hold values from -0.75 to 0.75
- diag_inverse: float32 [8, 2, 2, 256, 256], P('pole', None, None, 'blk'), may hold values from -6 to 6
- pole_weight: float32 [8, 2], P('pole'), may hold values from -4 to 4
- block_ids: int32 [128, 8], P(('pole', 'blk')), may hold values from 0 to 31, as said below
- block_count: int32 [128], P(('pole', 'blk')), may hold values from 1 to 8, 576 in all
- basis: float32 [128, 2048, 1024], P(('pole', 'blk')), may hold values from -0.1875 to 0.1875
- column_basis: float32 [128, 2048, 512], P(('pole', 'blk')), may hold values from -0.25 to 0.25
Outputs:
- diag_density: float32 [2, 256, 256], P(None, 'blk')
- density: float32 [128, 2048], P(('pole', 'blk'))
The draws below stay inside these ranges and needn't reach their ends.
Inputs may be any that keep to these rules, and one draw needn't show every extreme that they name: Entries of block_ids beyond a batch's block_count are not read; block_count reaches 8 in every draw. With b = g mod 16, every entry of block_ids[g] names a block of rows b' * 4096 // 16 to (b' + 1) * 4096 // 16 for some b' between b - 2 and b + 2.
All inputs are finite; a program needn't handle non-finite values. No bound on the sum of `block_count` on one device may be relied on, other than what follows from the above.
Results may differ from the reference program's by a relative error of at most 0.0003.
Values sent between devices are 32-bit elements; how exact they have to be, the bound alone decides.
A program may use at most 128 MiB of HBM per device.

```python
import math
import jax
import jax.numpy as jnp
import numpy as np
from jax import lax

M = 4096
K = 256
UPD = 2
RB = 128
MOST = 8
REACH = 2
PTS = 2048
POLES = 8
NBATCH = 128
COLS = 512
N_BLK = 16


def draw_block_ids(key, part):
    batch = jnp.arange(NBATCH, dtype=jnp.int32)[:, None]
    place = batch % N_BLK
    per_device = M // N_BLK // RB
    lowest = jnp.maximum(place - REACH, 0) * per_device
    highest = jnp.minimum(place + REACH + 1, N_BLK) * per_device
    raw = jax.random.randint(key, (NBATCH, MOST), 0, 1048576, dtype=jnp.int32)
    return (lowest + raw % (highest - lowest)).astype(jnp.int32)


def block_scale(stream_key, shape, split, low, high):
    level, own = 1.0, jax.random.fold_in(stream_key, 6)
    for dim, blocks in split:
        draws = jnp.exp(jax.random.uniform(jax.random.fold_in(own, dim), (blocks,), jnp.float32, low / len(split), high / len(split)))
        level = level * jnp.repeat(draws, shape[dim] // blocks).reshape([-1 if axis == dim else 1 for axis in range(len(shape))])
    return level


def split_up(count, total, reach, skew):
    loads = [(1 << 20) // math.isqrt(grade ** skew) + 1 for grade in range(2, count + 1)]
    surplus, given = total - reach - (count - 1), [1] * (count - 1)
    while surplus > 0:
        candidates = [i for i in range(count - 1) if given[i] < reach]
        mass, left = sum([loads[i] for i in candidates]), surplus
        for i in candidates:
            addition = min(reach - given[i], max(1, left * loads[i] // mass), surplus)
            given[i] = given[i] + addition
            surplus = surplus - addition
    return np.array([reach] + given)


def uneven(stream_key, count, total, bound, lean):
    if count == 2:
        one = jax.random.randint(stream_key, (), max(1, total - bound), min(bound, total - 1) + 1)
        return jnp.stack([one, total - one])
    tallies = jnp.asarray(split_up(count, total, bound, lean), jnp.int32)
    twos = (count - 1) // 2
    giver, sink = tallies[1:1 + 2 * twos:2], tallies[2:2 + 2 * twos:2]
    slack = jnp.minimum(giver - 1, bound - sink)
    passed = jax.random.randint(jax.random.fold_in(stream_key, 1), (twos,), 0, 1 << 20) % (slack + 1)
    tallies = tallies.at[1:1 + 2 * twos:2].set(giver - passed).at[2:2 + 2 * twos:2].set(sink + passed)
    return tallies[jax.random.permutation(jax.random.fold_in(stream_key, 2), count)]


def noise(key, shape, scale, reach, cuts=(), held_as=jnp.bfloat16):
    gain = block_scale(key, shape, cuts, -0.22, 0.18) if cuts else 1.0
    result = jax.random.normal(key, shape, jnp.float32) * scale * gain
    return jnp.minimum(jnp.maximum(result, -reach), reach).astype(held_as)


def setup_inputs(seed: int = 0) -> dict:
    key_list = jax.random.split(jax.random.key(seed), 9)
    inverse_block = noise(key_list[0], (POLES, 2, M, M), M ** -0.5, 0.09375, ((0, 8), (2, 16)), jnp.float32)
    factor = noise(key_list[1], (POLES, M, 2, COLS), 0.125, 0.75, ((0, 8), (1, 16)), jnp.float32)
    diag_inverse = noise(key_list[2], (POLES, 2, UPD, K, K), 1.0, 6.0, ((0, 8), (3, 16)), jnp.float32)
    pole_weight = noise(key_list[3], (POLES, 2), 1.0, 4.0, ((0, 8),), jnp.float32)
    block_ids = draw_block_ids(jax.random.fold_in(key_list[8], 71), 0)
    block_count = uneven(key_list[5], NBATCH, NBATCH * (MOST + 1) // 2, MOST, 2).astype(jnp.int32)
    basis = noise(key_list[6], (NBATCH, PTS, MOST * RB), (MOST * RB) ** -0.5, 0.1875, ((0, 128),), jnp.float32)
    column_basis = noise(key_list[7], (NBATCH, PTS, COLS), COLS ** -0.5, 0.25, ((0, 128),), jnp.float32)
    return {"inverse_block": inverse_block, "factor": factor, "diag_inverse": diag_inverse, "pole_weight": pole_weight, "block_ids": block_ids, "block_count": block_count, "basis": basis, "column_basis": column_basis}


HIGH = lax.Precision.HIGHEST


def matmul(left, right):
    return jnp.dot(left, right, preferred_element_type=jnp.float32, precision=HIGH)


def pair(left, right):
    return jnp.einsum('mjk,mjl->jkl', left, right, precision=HIGH)


def per_pole(items):
    block, panel, diag, weight = items
    real_g, imag_g = block[0], block[1]
    real_l, imag_l = panel[:, 0, :], panel[:, 1, :]
    real_x = -(matmul(real_g, real_l) - matmul(imag_g, imag_l))
    imag_x = -(matmul(real_g, imag_l) + matmul(imag_g, real_l))
    real_l3 = real_l.reshape(M, UPD, K)
    imag_l3 = imag_l.reshape(M, UPD, K)
    real_x3 = real_x.reshape(M, UPD, K)
    imag_x3 = imag_x.reshape(M, UPD, K)
    real_c = pair(real_l3, real_x3) - pair(imag_l3, imag_x3)
    imag_c = pair(real_l3, imag_x3) + pair(imag_l3, real_x3)
    real_s = diag[0] - real_c
    imag_s = diag[1] - imag_c
    part_matrix = weight[0] * real_x - weight[1] * imag_x
    part_diag = weight[0] * real_s - weight[1] * imag_s
    return part_matrix, part_diag


def reference(inverse_block, factor, diag_inverse, pole_weight, block_ids, block_count, basis, column_basis):
    parts_matrix, parts_diag = lax.map(per_pole, (inverse_block, factor, diag_inverse, pole_weight))
    matrix = jnp.sum(parts_matrix, axis=0)
    diag_density = jnp.sum(parts_diag, axis=0)
    blocks = matrix.reshape(M // RB, RB, UPD * K)

    def per_batch(items):
        ids, count, values, columns = items
        chosen = blocks[ids.astype(jnp.int32)]
        keep = (jnp.arange(MOST, dtype=jnp.int32) < count).astype(jnp.float32)
        selected = (chosen * keep[:, None, None]).reshape(MOST * RB, UPD * K)
        product = matmul(values, selected)
        return jnp.sum(product * columns, axis=-1)

    density = lax.map(per_batch, (block_ids, block_count, basis, column_basis))
    return diag_density, density
```

```python
import jax
import jax.numpy as jnp
from jax import lax
from jax.experimental import pallas as pl
from jax.experimental.pallas import tpu as pltpu
from jax.sharding import PartitionSpec as P

MESH = pl.DeviceIdType.MESH
F32 = jnp.float32
BF16 = jnp.bfloat16
CH = 4
REACH = 2


def split(x):
    high = x.astype(BF16)
    return high, (x - high.astype(F32)).astype(BF16)


def dot(a, b):
    return jnp.dot(a, b, preferred_element_type=F32)


def dot3(ah, al, bh, bl):
    return dot(ah, bh) + dot(ah, bl) + dot(al, bh)


def kernel(
    w_ref, ids_ref, cnt_ref, g_ref, l_ref, d_ref, basis_ref, cb_ref,
    diag_ref, dens_ref,
    lbuf, gh, gl, stage, bh, bl, cbuf, mbuf, ybuf, rsb, sb, zb, dpart, dgb, dpb, dsum,
    acc, dacc, selh, lth, ltl, dv, mloc,
    ag_s, ag_r, co_s, co_r, rs_s, rs_r, zl_s, zl_r, re_s, re_r, ax_s, ax_r,
    dg_s, dg_r, dp_s, dp_r, st_sem, loc_sem, cb_sem,
):
    p = lax.axis_index("pole")
    b = lax.axis_index("blk")
    x, zl = p // 2, lax.rem(p, 2)
    y, zh, co = b // 4, lax.rem(b // 2, 2), lax.rem(b, 2)
    oz, oc = 1 - zh, 1 - co
    yu, yd, yo = lax.rem(y + 1, 4), lax.rem(y + 3, 4), lax.rem(y + 2, 4)

    def at(yy, zz, cc):
        return yy * 4 + zz * 2 + cc

    up, down, over, sib = (p, at(yu, zh, co)), (p, at(yd, zh, co)), (p, at(y, oz, co)), (p, at(y, zh, oc))

    own = [pltpu.make_async_copy(l_ref.at[c], lbuf.at[c, b], loc_sem.at[c]) for c in range(CH)]
    for cp in own:
        cp.start()
    dcopy = pltpu.make_async_copy(d_ref, dv, loc_sem.at[CH])
    dcopy.start()

    def g_copy(i):
        return pltpu.make_async_copy(
            g_ref.at[i // 16, :, pl.ds(pl.multiple_of(lax.rem(i, 16) * 256, 256), 256)], stage.at[i], st_sem.at[i])

    def b_copy(i):
        return pltpu.make_async_copy(
            basis_ref.at[pl.ds(pl.multiple_of((i // 4) * 256, 256), 256),
                         pl.ds(pl.multiple_of(lax.rem(i, 4) * 256, 256), 256)], stage.at[i], st_sem.at[i])

    @pl.loop(0, 32)
    def _(i):
        g_copy(i).start()

    bar = pltpu.get_barrier_semaphore()

    @pl.loop(1, 16)
    def _(d):
        pl.semaphore_signal(bar, inc=1, device_id=(p, lax.rem(b + d, 16)), device_id_type=MESH)

    @pl.loop(1, 8)
    def _(d):
        pl.semaphore_signal(bar, inc=1, device_id=(lax.rem(p + d, 8), b), device_id_type=MESH)

    for cp in own:
        cp.wait()
    pl.semaphore_wait(bar, 22)

    def rc(src, dst, s, r, dev):
        return pltpu.make_async_remote_copy(src, dst, s, r, device_id=dev, device_id_type=MESH)

    def ag(c, kind, slot, dev, rows=None):
        ref = lbuf.at[c, slot] if rows is None else lbuf.at[c, slot, pl.ds(rows, 128)]
        return rc(ref, ref, ag_s.at[c, kind], ag_r.at[c, kind], dev)

    def cf(c, i, slot):
        ref = lbuf.at[c, slot]
        return rc(ref, ref, co_s.at[c, i], co_r.at[c, i], sib)

    def slot_of(i, cc):
        return at(lax.rem(y + lax.rem(i, 4), 4), lax.rem(zh + i // 4, 2), cc)

    def send_own(c):
        ag(c, 0, b, up).start()
        ag(c, 1, b, down).start()
        ag(c, 2, b, over).start()
        cf(c, 0, b).start()

    s1, s2, s3, s4 = at(yd, zh, co), at(yu, zh, co), at(y, oz, co), at(yo, zh, co)
    s5, s6, s7 = at(yd, oz, co), at(yu, oz, co), at(yo, oz, co)

    def early(c, ahead):
        ag(c, 0, s1, up).wait_recv()
        ag(c, 3, s1, up, 0).start()
        cf(c, 3, s1).start()
        ag(c, 1, s2, down).wait_recv()
        ag(c, 4, s2, down, 128).start()
        cf(c, 1, s2).start()
        ag(c, 2, s3, over).wait_recv()
        ag(c, 5, s3, up).start()
        ag(c, 6, s3, down).start()
        cf(c, 4, s3).start()
        ahead()

    def middle(c):
        ag(c, 3, s4, up, 0).wait_recv()
        ag(c, 7, s4, over, 0).start()
        ag(c, 4, s4, down, 128).wait_recv()
        ag(c, 8, s4, over, 128).start()
        cf(c, 2, s4).start()

    def late(c):
        ag(c, 5, s5, up).wait_recv()
        cf(c, 7, s5).start()
        ag(c, 6, s6, down).wait_recv()
        cf(c, 5, s6).start()
        ag(c, 7, s7, over, 0).wait_recv()
        ag(c, 8, s7, over, 128).wait_recv()
        cf(c, 6, s7).start()

    def piece(c, slot):
        v = lbuf[c, slot]
        h, l = split(v)
        h2 = jnp.concatenate([-h[:, 128:], h[:, :128]], axis=1)
        l2 = jnp.concatenate([-l[:, 128:], l[:, :128]], axis=1)
        return dot3(gh[slot], gl[slot], h, l) + dot3(gh[16 + slot], gl[16 + slot], h2, l2)

    def products(c, low, high):
        @pl.loop(low, high)
        def _(i):
            acc[...] += piece(c, slot_of(i, co))
            o = slot_of(i, oc)
            cf(c, i, o).wait_recv()
            acc[...] += piece(c, o)

    wr, wi = w_ref[0, 0], w_ref[0, 1]

    def t1(c):
        a = acc[...]
        ar, ai = a[:, :128], a[:, 128:]
        yr, yi = wi * ai - wr * ar, -(wr * ai + wi * ar)
        ybuf[c] = yr
        for d in range(1, 4):
            xx = lax.rem(x + d, 4)
            rc(ybuf.at[c, pl.ds(pl.multiple_of(xx * 64, 64), 64)], rsb.at[c, d], rs_s.at[c, d], rs_r.at[c, d],
               (xx * 2 + zl, b)).start()
        yrh, yrl = split(yr)
        yih, yil = split(yi)
        j = 2 * (c // 2)
        for h in range(2):
            th, tl = lth[j + h], ltl[j + h]
            dpart[c, pl.ds(h * 128, 128)] = dot3(th[:128], tl[:128], yrh, yrl) - dot3(th[128:], tl[128:], yih, yil)

    def t1b(c):
        tot = ybuf[c, pl.ds(pl.multiple_of(x * 64, 64), 64)]
        for d in range(1, 4):
            rc(rsb.at[c, d], rsb.at[c, d], rs_s.at[c, d], rs_r.at[c, d], sib).wait_recv()
            tot = tot + rsb[c, d]
        sb[c] = tot
        rc(sb.at[c], zb.at[c], zl_s.at[c], zl_r.at[c], (x * 2 + 1 - zl, b)).start()

    def t2(c):
        rc(sb.at[c], zb.at[c], zl_s.at[c], zl_r.at[c], sib).wait_recv()
        mbuf[c, REACH, x] = sb[c] + zb[c]
        for off in (2, -2, 1, -1):
            k = REACH - off
            rc(mbuf.at[c, REACH, x], mbuf.at[c, k, x], re_s.at[c, k], re_r.at[c, k],
               (p, lax.rem(b + 16 + off, 16))).start()

    def t3(c):
        for k in (0, 1, 3, 4):
            rc(mbuf.at[c, k, x], mbuf.at[c, k, x], re_s.at[c, k], re_r.at[c, k], sib).wait_recv()
        for d in range(1, 4):
            rc(mbuf.at[c, :, x], mbuf.at[c, :, x], ax_s.at[c, d], ax_r.at[c, d],
               (lax.rem(x + d, 4) * 2 + zl, b)).start()

    def t4(c):
        for d in range(1, 4):
            xx = lax.rem(x + 4 - d, 4)
            rc(mbuf.at[c, :, xx], mbuf.at[c, :, xx], ax_s.at[c, d], ax_r.at[c, d], sib).wait_recv()
        for k in range(2 * REACH + 1):
            for q in range(4):
                mloc[k * 4 + q] = mbuf[c, k, q]
        count = cnt_ref[0]
        first = (b - REACH) * 2

        @pl.loop(0, 8)
        def _(s):
            n = jnp.clip(ids_ref[0, s] - first, 0, 4 * REACH + 1)
            keep = jnp.where(s < count, 1.0, 0.0).astype(F32)
            for i in range(2):
                h, l = split(mloc[n * 2 + i] * keep)
                rows = pl.ds(pl.multiple_of(s * 128 + i * 64, 64), 64)
                selh[rows, :128] = h
                selh[rows, 128:] = l

        @pl.loop(0, 8)
        def _(r):
            pq = dot(bh[r], selh[...])
            q = dot(bl[r], selh[:, :128])
            rows = pl.ds(pl.multiple_of(r * 256, 256), 256)
            dacc[rows] += (pq[:, :128] + pq[:, 128:] + q) * cbuf[c, rows]

    send_own(0)
    send_own(1)

    @pl.loop(0, 32)
    def _(i):
        g_copy(i).wait()
        h, l = split(stage[i])
        gh[i] = h
        gl[i] = l
        b_copy(i).start()

    for c in range(CH):
        pltpu.make_async_copy(cb_ref.at[:, pl.ds(c * 128, 128)], cbuf.at[c], cb_sem.at[c]).start()

    @pl.loop(0, CH)
    def _(c):
        h, l = split(lbuf[c, b].T)
        lth[c] = h
        ltl[c] = l

    early(0, lambda: send_own(2))

    @pl.loop(0, 32)
    def _(i):
        b_copy(i).wait()
        h, l = split(stage[i])
        bh[i // 4, :, pl.ds(pl.multiple_of(lax.rem(i, 4) * 256, 256), 256)] = h
        bl[i // 4, :, pl.ds(pl.multiple_of(lax.rem(i, 4) * 256, 256), 256)] = l

    for c in range(CH):
        pltpu.make_async_copy(cb_ref.at[:, pl.ds(c * 128, 128)], cbuf.at[c], cb_sem.at[c]).wait()
    dcopy.wait()
    dacc[...] = jnp.zeros_like(dacc)

    @pl.loop(0, CH)
    def _(c):
        @pl.when(c < CH - 1)
        def _():
            def ahead():
                @pl.when(c + 3 < CH)
                def _():
                    send_own(c + 3)

            early(c + 1, ahead)

        @pl.when(c > 0)
        def _():
            t1b(c - 1)

        middle(c)
        acc[...] = jnp.zeros_like(acc)
        products(c, 0, 5)

        @pl.when(c > 0)
        def _():
            t2(c - 1)

        late(c)
        products(c, 5, 8)
        t1(c)

        @pl.when(c > 0)
        def _():
            t3(c - 1)
            t4(c - 1)

    last = CH - 1
    t1b(last)
    t2(last)

    def dg(d, row):
        return rc(dpart.at[:, pl.ds(pl.multiple_of(row * 16, 16), 16)], dgb.at[d], dg_s.at[d], dg_r.at[d],
                  (p, lax.rem(b + d, 16)))

    @pl.loop(1, 16)
    def _(d):
        dg(d, lax.rem(b + d, 16)).start()

    t3(last)

    dsum[...] = dpart[:, pl.ds(pl.multiple_of(b * 16, 16), 16)]

    @pl.loop(1, 16)
    def _(d):
        dg(d, 0).wait_recv()
        dsum[...] += dgb[d]

    for c in range(CH):
        cols = slice((c % 2) * 128, (c % 2) * 128 + 128)
        dsum[c] = wr * dv[0, c // 2, :, cols] - wi * dv[1, c // 2, :, cols] - dsum[c]

    def dp(d):
        return rc(dsum, dpb.at[d], dp_s.at[d], dp_r.at[d], (lax.rem(p + d, 8), b))

    @pl.loop(1, 8)
    def _(d):
        dp(d).start()

    t4(last)

    for r in range(16):
        dens_ref[r, :] = jnp.sum(dacc[r * 128 : (r + 1) * 128].T, axis=0)

    dpb[0] = dsum[...]

    @pl.loop(1, 8)
    def _(d):
        dp(d).wait_recv()
        dpb[0] += dpb[d]

    for c in range(CH):
        diag_ref[c // 2, :, (c % 2) * 128 : (c % 2) * 128 + 128] = dpb[0, c]

    @pl.loop(0, CH)
    def _(c):
        for kind in range(9):
            rows = {3: 0, 4: 128, 7: 0, 8: 128}.get(kind)
            ag(c, kind, b, sib, rows).wait_send()
        for i in range(8):
            cf(c, i, b).wait_send()
        for d in range(1, 4):
            rc(rsb.at[c, d], rsb.at[c, d], rs_s.at[c, d], rs_r.at[c, d], sib).wait_send()
            rc(mbuf.at[c, :, x], mbuf.at[c, :, x], ax_s.at[c, d], ax_r.at[c, d], sib).wait_send()
        rc(sb.at[c], zb.at[c], zl_s.at[c], zl_r.at[c], sib).wait_send()
        for k in (0, 1, 3, 4):
            rc(mbuf.at[c, k, x], mbuf.at[c, k, x], re_s.at[c, k], re_r.at[c, k], sib).wait_send()

    @pl.loop(1, 16)
    def _(d):
        dg(d, 0).wait_send()

    @pl.loop(1, 8)
    def _(d):
        dp(d).wait_send()


def body(inverse_block, factor, diag_inverse, pole_weight, block_ids, block_count, basis, column_basis):
    panels = factor[0].reshape(256, 2, CH, 128).transpose(2, 0, 1, 3).reshape(CH, 256, 256)
    dma = pltpu.SemaphoreType.DMA
    anyspace = pl.BlockSpec(memory_space=pl.ANY)
    smem = pl.BlockSpec(memory_space=pltpu.SMEM)
    vmem = pl.BlockSpec(memory_space=pltpu.VMEM)
    diag, dens = pl.pallas_call(
        kernel,
        name="selinv",
        out_shape=(jax.ShapeDtypeStruct((2, 16, 256), F32), jax.ShapeDtypeStruct((16, 128), F32)),
        in_specs=[smem, smem, smem, anyspace, anyspace, anyspace, anyspace, anyspace],
        out_specs=(vmem, vmem),
        scratch_shapes=[
            pltpu.VMEM((CH, 16, 256, 256), F32),
            pltpu.VMEM((32, 256, 256), BF16),
            pltpu.VMEM((32, 256, 256), BF16),
            pltpu.VMEM((32, 256, 256), F32),
            pltpu.VMEM((8, 256, 1024), BF16),
            pltpu.VMEM((8, 256, 1024), BF16),
            pltpu.VMEM((CH, 2048, 128), F32),
            pltpu.VMEM((CH, 5, 4, 64, 128), F32),
            pltpu.VMEM((CH, 256, 128), F32),
            pltpu.VMEM((CH, 4, 64, 128), F32),
            pltpu.VMEM((CH, 64, 128), F32),
            pltpu.VMEM((CH, 64, 128), F32),
            pltpu.VMEM((CH, 256, 128), F32),
            pltpu.VMEM((16, CH, 16, 128), F32),
            pltpu.VMEM((8, CH, 16, 128), F32),
            pltpu.VMEM((CH, 16, 128), F32),
            pltpu.VMEM((256, 256), F32),
            pltpu.VMEM((2048, 128), F32),
            pltpu.VMEM((1024, 256), BF16),
            pltpu.VMEM((CH, 256, 256), BF16),
            pltpu.VMEM((CH, 256, 256), BF16),
            pltpu.VMEM((2, 2, 16, 256), F32),
            pltpu.VMEM((20, 64, 128), F32),
            dma((CH, 9)), dma((CH, 9)), dma((CH, 8)), dma((CH, 8)),
            dma((CH, 4)), dma((CH, 4)), dma((CH,)), dma((CH,)), dma((CH, 5)), dma((CH, 5)), dma((CH, 4)), dma((CH, 4)),
            dma((16,)), dma((16,)), dma((8,)), dma((8,)), dma((32,)), dma((CH + 1,)), dma((CH,)),
        ],
        compiler_params=pltpu.CompilerParams(
            collective_id=0, has_side_effects=True, vmem_limit_bytes=67_000_000),
    )(pole_weight, block_ids, block_count,
      inverse_block[0], panels, diag_inverse[0], basis[0], column_basis[0])
    return diag, dens.reshape(1, 2048)


def solution(mesh):
    in_specs = (
        P("pole", None, "blk", None),
        P("pole", "blk", None, None),
        P("pole", None, None, "blk", None),
        P("pole", None),
        P(("pole", "blk"), None),
        P(("pole", "blk")),
        P(("pole", "blk"), None, None),
        P(("pole", "blk"), None, None),
    )
    out_specs = (P(None, "blk", None), P(("pole", "blk"), None))
    return jax.shard_map(body, mesh=mesh, in_specs=in_specs, out_specs=out_specs, check_vma=False)
```

```python
import jax
import jax.numpy as jnp
from jax import lax
from jax.experimental import pallas as pl
from jax.experimental.pallas import tpu as pltpu
from jax.sharding import PartitionSpec as P

MESH = pl.DeviceIdType.MESH
F32 = jnp.float32
BF16 = jnp.bfloat16
CH = 4
REACH = 2


ORDER = (
    "E0Z0C0Y2V2E1Z1F0",
    "P0Y3H0Q0V3F1E2Z2",
    "P110H1Q1F2E3Z3P2",
    "2011H2Q230F3P321",
    "H3Q312B031132240",
    "23B1D03233S041B2",
    "42B343",
)


def events():
    text = "".join(ORDER)
    return [(text[i], int(text[i + 1])) for i in range(0, len(text), 2)]


def split(x):
    high = x.astype(BF16)
    return high, (x - high.astype(F32)).astype(BF16)


def dot(a, b):
    return jnp.dot(a, b, preferred_element_type=F32)


def dot3(ah, al, bh, bl):
    return dot(ah, bh) + dot(ah, bl) + dot(al, bh)


def kernel(
    w_ref, ids_ref, cnt_ref, g_ref, l_ref, d_ref, basis_ref, cb_ref,
    diag_ref, dens_ref,
    lbuf, gh, gl, stage, bh, bl, cbuf, mbuf, ybuf, rsb, sb, zb, dpart, dgb, dpb, dsum,
    acc, dacc, selh, lth, ltl, dv, mloc,
    ag_s, ag_r, co_s, co_r, rs_s, rs_r, zl_s, zl_r, re_s, re_r, ax_s, ax_r, sx_s, sx_r,
    dg_s, dg_r, dp_s, dp_r, st_sem, own_sem, loc_sem, cb_sem,
):
    p = lax.axis_index("pole")
    b = lax.axis_index("blk")
    x, zl = p // 2, lax.rem(p, 2)
    y, zh, co = b // 4, lax.rem(b // 2, 2), lax.rem(b, 2)
    oz, oc = 1 - zh, 1 - co
    yu, yd, yo = lax.rem(y + 1, 4), lax.rem(y + 3, 4), lax.rem(y + 2, 4)

    def at(yy, zz, cc):
        return yy * 4 + zz * 2 + cc

    up, down, over, sib = (p, at(yu, zh, co)), (p, at(yd, zh, co)), (p, at(y, oz, co)), (p, at(y, zh, oc))

    own = [
        pltpu.make_async_copy(
            l_ref.at[:, k, pl.ds(c * 128, 128)], lbuf.at[c, b, :, pl.ds(k * 128, 128)], own_sem.at[c, k])
        for c in range(CH) for k in range(2)
    ]
    for cp in own:
        cp.start()
    dcopy = pltpu.make_async_copy(d_ref, dv, loc_sem.at[0])
    dcopy.start()

    def g_copy(i):
        return pltpu.make_async_copy(
            g_ref.at[i // 16, :, pl.ds(pl.multiple_of(lax.rem(i, 16) * 256, 256), 256)], stage.at[i], st_sem.at[i])

    def b_copy(i):
        return pltpu.make_async_copy(
            basis_ref.at[pl.ds(pl.multiple_of((i // 4) * 256, 256), 256),
                         pl.ds(pl.multiple_of(lax.rem(i, 4) * 256, 256), 256)], stage.at[i], st_sem.at[i])

    @pl.loop(0, 32)
    def _(i):
        g_copy(i).start()

    bar = pltpu.get_barrier_semaphore()

    @pl.loop(1, 16)
    def _(d):
        pl.semaphore_signal(bar, inc=1, device_id=(p, lax.rem(b + d, 16)), device_id_type=MESH)

    @pl.loop(1, 8)
    def _(d):
        pl.semaphore_signal(bar, inc=1, device_id=(lax.rem(p + d, 8), b), device_id_type=MESH)

    pl.semaphore_wait(bar, 22)
    for cp in own:
        cp.wait()

    def rc(src, dst, s, r, dev):
        return pltpu.make_async_remote_copy(src, dst, s, r, device_id=dev, device_id_type=MESH)

    def ag(c, kind, slot, dev, rows=None):
        ref = lbuf.at[c, slot] if rows is None else lbuf.at[c, slot, pl.ds(rows, 128)]
        return rc(ref, ref, ag_s.at[c, kind], ag_r.at[c, kind], dev)

    def cf(c, i, slot):
        ref = lbuf.at[c, slot]
        return rc(ref, ref, co_s.at[c, i], co_r.at[c, i], sib)

    def slot_of(i, cc):
        return at(lax.rem(y + lax.rem(i, 4), 4), lax.rem(zh + i // 4, 2), cc)

    def own_y(c):
        ag(c, 0, b, up).start()
        ag(c, 1, b, down).start()
        cf(c, 0, b).start()

    def own_z(c):
        ag(c, 2, b, over).start()

    s1, s2, s3, s4 = at(yd, zh, co), at(yu, zh, co), at(y, oz, co), at(yo, zh, co)
    s5, s6, s7 = at(yd, oz, co), at(yu, oz, co), at(yo, oz, co)

    def ring(c):
        ag(c, 0, s1, up).wait_recv()
        ag(c, 3, s1, up, 0).start()
        cf(c, 3, s1).start()
        ag(c, 1, s2, down).wait_recv()
        ag(c, 4, s2, down, 128).start()
        cf(c, 1, s2).start()

    def across(c):
        ag(c, 2, s3, over).wait_recv()
        ag(c, 5, s3, up).start()
        ag(c, 6, s3, down).start()
        cf(c, 4, s3).start()

    def far(c):
        ag(c, 3, s4, up, 0).wait_recv()
        ag(c, 7, s4, over, 0).start()
        ag(c, 4, s4, down, 128).wait_recv()
        ag(c, 8, s4, over, 128).start()
        cf(c, 2, s4).start()

    def late(c):
        ag(c, 5, s5, up).wait_recv()
        cf(c, 7, s5).start()
        ag(c, 6, s6, down).wait_recv()
        cf(c, 5, s6).start()
        ag(c, 7, s7, over, 0).wait_recv()
        ag(c, 8, s7, over, 128).wait_recv()
        cf(c, 6, s7).start()

    def piece(c, slot):
        v = lbuf[c, slot]
        h, l = split(v)
        h2 = jnp.concatenate([-h[:, 128:], h[:, :128]], axis=1)
        l2 = jnp.concatenate([-l[:, 128:], l[:, :128]], axis=1)
        return dot3(gh[slot], gl[slot], h, l) + dot3(gh[16 + slot], gl[16 + slot], h2, l2)

    def products(c, low, high):
        @pl.loop(low, high)
        def _(i):
            acc[...] += piece(c, slot_of(i, co))
            o = slot_of(i, oc)
            cf(c, i, o).wait_recv()
            acc[...] += piece(c, o)

    wr, wi = w_ref[0, 0], w_ref[0, 1]

    def t1(c):
        a = acc[...]
        ar, ai = a[:, :128], a[:, 128:]
        yr, yi = wi * ai - wr * ar, -(wr * ai + wi * ar)
        ybuf[c] = yr
        for d in range(1, 4):
            xx = lax.rem(x + d, 4)
            rc(ybuf.at[c, pl.ds(pl.multiple_of(xx * 64, 64), 64)], rsb.at[c, d], rs_s.at[c, d], rs_r.at[c, d],
               (xx * 2 + zl, b)).start()
        yrh, yrl = split(yr)
        yih, yil = split(yi)
        j = 2 * (c // 2)
        for h in range(2):
            th, tl = lth[j + h], ltl[j + h]
            dpart[c, pl.ds(h * 128, 128)] = dot3(th[:128], tl[:128], yrh, yrl) - dot3(th[128:], tl[128:], yih, yil)

    def t1b(c):
        tot = ybuf[c, pl.ds(pl.multiple_of(x * 64, 64), 64)]
        for d in range(1, 4):
            rc(rsb.at[c, d], rsb.at[c, d], rs_s.at[c, d], rs_r.at[c, d], sib).wait_recv()
            tot = tot + rsb[c, d]
        sb[c] = tot
        rc(sb.at[c], zb.at[c], zl_s.at[c], zl_r.at[c], (x * 2 + 1 - zl, b)).start()

    mine = pl.ds(3 * co, 3)
    theirs = pl.ds(3 * oc, 3)

    def t2(c):
        rc(sb.at[c], zb.at[c], zl_s.at[c], zl_r.at[c], sib).wait_recv()
        mbuf[c, 2 + co, x] = sb[c] + zb[c]
        src = mbuf.at[c, 2 + co, x]
        rc(src, mbuf.at[c, co, x], re_s.at[c, 0], re_r.at[c, co], (p, lax.rem(b + 2 - co, 16))).start()
        rc(src, mbuf.at[c, 4 + co, x], re_s.at[c, 1], re_r.at[c, co], (p, lax.rem(b + 15 - co, 16))).start()

    def sx(c, d, xx, part):
        return rc(mbuf.at[c, part, xx], mbuf.at[c, part, xx], sx_s.at[c, d], sx_r.at[c, d], sib)

    def t3(c):
        for r in range(2):
            got = mbuf.at[c, r + 4 * co, x]
            rc(got, got, re_s.at[c, r], re_r.at[c, r], sib).wait_recv()
        part = mbuf.at[c, mine, x]
        for d in (2, 1, 3):
            rc(part, part, ax_s.at[c, d], ax_r.at[c, d], (lax.rem(x + d, 4) * 2 + zl, b)).start()
        sx(c, 0, x, mine).start()

    def t3b(c):
        for d in (1, 3, 2):
            xx = lax.rem(x + 4 - d, 4)
            part = mbuf.at[c, mine, xx]
            rc(part, part, ax_s.at[c, d], ax_r.at[c, d], sib).wait_recv()
            sx(c, d, xx, mine).start()

    def t4(c):
        for d in (0, 1, 3, 2):
            sx(c, d, lax.rem(x + 4 - d, 4), theirs).wait_recv()
        for k in range(6):
            for q in range(4):
                mloc[k * 4 + q] = mbuf[c, k, q]
        count = cnt_ref[0]
        first = (b - co - REACH) * 2

        @pl.loop(0, 8)
        def _(s):
            n = jnp.clip(ids_ref[0, s] - first, 0, 11)
            keep = jnp.where(s < count, 1.0, 0.0).astype(F32)
            for i in range(2):
                h, l = split(mloc[n * 2 + i] * keep)
                rows = pl.ds(pl.multiple_of(s * 128 + i * 64, 64), 64)
                selh[rows, :128] = h
                selh[rows, 128:] = l

        @pl.loop(0, 8)
        def _(r):
            pq = dot(bh[r], selh[...])
            q = dot(bl[r], selh[:, :128])
            rows = pl.ds(pl.multiple_of(r * 256, 256), 256)
            dacc[rows] += (pq[:, :128] + pq[:, 128:] + q) * cbuf[c, rows]

    def begin(c):
        acc[...] = jnp.zeros_like(acc)
        products(c, 0, 5)

    def finish(c):
        products(c, 5, 8)
        t1(c)

    steps = {"Y": own_y, "V": own_z, "E": ring, "Z": across, "F": far, "H": late, "P": begin, "Q": finish,
             "1": t1b, "2": t2, "3": t3, "B": t3b, "4": t4}

    own_y(0)
    own_z(0)
    own_y(1)
    own_z(1)

    @pl.loop(0, 32)
    def _(i):
        g_copy(i).wait()
        h, l = split(stage[i])
        gh[i] = h
        gl[i] = l
        b_copy(i).start()

    for c in range(CH):
        pltpu.make_async_copy(cb_ref.at[:, pl.ds(c * 128, 128)], cbuf.at[c], cb_sem.at[c]).start()

    @pl.loop(0, CH)
    def _(c):
        h, l = split(lbuf[c, b].T)
        lth[c] = h
        ltl[c] = l

    def basis_split(_):
        @pl.loop(0, 32)
        def _(i):
            b_copy(i).wait()
            h, l = split(stage[i])
            bh[i // 4, :, pl.ds(pl.multiple_of(lax.rem(i, 4) * 256, 256), 256)] = h
            bl[i // 4, :, pl.ds(pl.multiple_of(lax.rem(i, 4) * 256, 256), 256)] = l

        for c in range(CH):
            pltpu.make_async_copy(cb_ref.at[:, pl.ds(c * 128, 128)], cbuf.at[c], cb_sem.at[c]).wait()
        dcopy.wait()
        dacc[...] = jnp.zeros_like(dacc)

    def dg(d, row):
        return rc(dpart.at[:, pl.ds(pl.multiple_of(row * 16, 16), 16)], dgb.at[d], dg_s.at[d], dg_r.at[d],
                  (p, lax.rem(b + d, 16)))

    def dp(d):
        return rc(dsum, dpb.at[d], dp_s.at[d], dp_r.at[d], (lax.rem(p + d, 8), b))

    def diag_send(_):
        @pl.loop(1, 16)
        def _(d):
            dg(d, lax.rem(b + d, 16)).start()

    def diag_sum(_):
        dsum[...] = dpart[:, pl.ds(pl.multiple_of(b * 16, 16), 16)]

        @pl.loop(1, 16)
        def _(d):
            dg(d, 0).wait_recv()
            dsum[...] += dgb[d]

        for c in range(CH):
            cols = slice((c % 2) * 128, (c % 2) * 128 + 128)
            dsum[c] = wr * dv[0, c // 2, :, cols] - wi * dv[1, c // 2, :, cols] - dsum[c]

        @pl.loop(1, 8)
        def _(d):
            dp(d).start()

    steps.update({"C": basis_split, "D": diag_send, "S": diag_sum})

    for ev, c in events():
        steps[ev](c)

    for r in range(16):
        dens_ref[r, :] = jnp.sum(dacc[r * 128 : (r + 1) * 128].T, axis=0)

    dpb[0] = dsum[...]

    @pl.loop(1, 8)
    def _(d):
        dp(d).wait_recv()
        dpb[0] += dpb[d]

    for c in range(CH):
        diag_ref[c // 2, :, (c % 2) * 128 : (c % 2) * 128 + 128] = dpb[0, c]

    @pl.loop(0, CH)
    def _(c):
        for kind in range(9):
            rows = {3: 0, 4: 128, 7: 0, 8: 128}.get(kind)
            ag(c, kind, b, sib, rows).wait_send()
        for i in range(8):
            cf(c, i, b).wait_send()
        for d in range(1, 4):
            rc(rsb.at[c, d], rsb.at[c, d], rs_s.at[c, d], rs_r.at[c, d], sib).wait_send()
            rc(mbuf.at[c, mine, x], mbuf.at[c, mine, x], ax_s.at[c, d], ax_r.at[c, d], sib).wait_send()
        rc(sb.at[c], zb.at[c], zl_s.at[c], zl_r.at[c], sib).wait_send()
        for k in range(2):
            rc(mbuf.at[c, k, x], mbuf.at[c, k, x], re_s.at[c, k], re_r.at[c, k], sib).wait_send()
        for d in range(4):
            sx(c, d, x, mine).wait_send()

    @pl.loop(1, 16)
    def _(d):
        dg(d, 0).wait_send()

    @pl.loop(1, 8)
    def _(d):
        dp(d).wait_send()


def body(inverse_block, factor, diag_inverse, pole_weight, block_ids, block_count, basis, column_basis):
    dma = pltpu.SemaphoreType.DMA
    anyspace = pl.BlockSpec(memory_space=pl.ANY)
    smem = pl.BlockSpec(memory_space=pltpu.SMEM)
    vmem = pl.BlockSpec(memory_space=pltpu.VMEM)
    diag, dens = pl.pallas_call(
        kernel,
        name="selinv",
        out_shape=(jax.ShapeDtypeStruct((2, 16, 256), F32), jax.ShapeDtypeStruct((16, 128), F32)),
        in_specs=[smem, smem, smem, anyspace, anyspace, anyspace, anyspace, anyspace],
        out_specs=(vmem, vmem),
        scratch_shapes=[
            pltpu.VMEM((CH, 16, 256, 256), F32),
            pltpu.VMEM((32, 256, 256), BF16),
            pltpu.VMEM((32, 256, 256), BF16),
            pltpu.VMEM((32, 256, 256), F32),
            pltpu.VMEM((8, 256, 1024), BF16),
            pltpu.VMEM((8, 256, 1024), BF16),
            pltpu.VMEM((CH, 2048, 128), F32),
            pltpu.VMEM((CH, 6, 4, 64, 128), F32),
            pltpu.VMEM((CH, 256, 128), F32),
            pltpu.VMEM((CH, 4, 64, 128), F32),
            pltpu.VMEM((CH, 64, 128), F32),
            pltpu.VMEM((CH, 64, 128), F32),
            pltpu.VMEM((CH, 256, 128), F32),
            pltpu.VMEM((16, CH, 16, 128), F32),
            pltpu.VMEM((8, CH, 16, 128), F32),
            pltpu.VMEM((CH, 16, 128), F32),
            pltpu.VMEM((256, 256), F32),
            pltpu.VMEM((2048, 128), F32),
            pltpu.VMEM((1024, 256), BF16),
            pltpu.VMEM((CH, 256, 256), BF16),
            pltpu.VMEM((CH, 256, 256), BF16),
            pltpu.VMEM((2, 2, 16, 256), F32),
            pltpu.VMEM((24, 64, 128), F32),
            dma((CH, 9)), dma((CH, 9)), dma((CH, 8)), dma((CH, 8)),
            dma((CH, 4)), dma((CH, 4)), dma((CH,)), dma((CH,)), dma((CH, 2)), dma((CH, 2)), dma((CH, 4)), dma((CH, 4)), dma((CH, 4)), dma((CH, 4)),
            dma((16,)), dma((16,)), dma((8,)), dma((8,)), dma((32,)), dma((CH, 2)), dma((1,)), dma((CH,)),
        ],
        compiler_params=pltpu.CompilerParams(
            collective_id=0, has_side_effects=True, vmem_limit_bytes=67_000_000),
    )(pole_weight, block_ids, block_count,
      inverse_block[0], factor[0], diag_inverse[0], basis[0], column_basis[0])
    return diag, dens.reshape(1, 2048)


def solution(mesh):
    in_specs = (
        P("pole", None, "blk", None),
        P("pole", "blk", None, None),
        P("pole", None, None, "blk", None),
        P("pole", None),
        P(("pole", "blk"), None),
        P(("pole", "blk")),
        P(("pole", "blk"), None, None),
        P(("pole", "blk"), None, None),
    )
    out_specs = (P(None, "blk", None), P(("pole", "blk"), None))
    return jax.shard_map(body, mesh=mesh, in_specs=in_specs, out_specs=out_specs, check_vma=False)
```

```python
import jax
import jax.numpy as jnp
from jax import lax
from jax.experimental import pallas as pl
from jax.experimental.pallas import tpu as pltpu
from jax.sharding import PartitionSpec as P

MESH = pl.DeviceIdType.MESH
F32 = jnp.float32
BF16 = jnp.bfloat16
CH = 4
REACH = 2


ORDER = (
    "E0Z0C0Y2V2E1Z1F0",
    "P0Y3H0Q0V3F1E2Z2",
    "P110H1Q1F2E3Z3P2",
    "2011H2Q230F3P3H3",
    "Q31221132231B023",
    "403233B1D041B242",
    "B3S043",
)


def events():
    text = "".join(ORDER)
    return [(text[i], int(text[i + 1])) for i in range(0, len(text), 2)]


def split(x):
    high = x.astype(BF16)
    return high, (x - high.astype(F32)).astype(BF16)


def dot(a, b):
    return jnp.dot(a, b, preferred_element_type=F32)


def dot3(ah, al, bh, bl):
    return dot(ah, bh) + dot(ah, bl) + dot(al, bh)


def kernel(
    w_ref, ids_ref, cnt_ref, g_ref, l_ref, d_ref, basis_ref, cb_ref,
    diag_ref, dens_ref,
    lbuf, gh, gl, stage, bh, bl, cbuf, mbuf, ybuf, rsb, sb, zb, dpart, dgb, dpb, dsum,
    acc, dacc, selh, lth, ltl, dv, mloc,
    ag_s, ag_r, co_s, co_r, rs_s, rs_r, zl_s, zl_r, re_s, re_r, ao_s, ao_r, ax_s, ax_r, sx_s, sx_r,
    dg_s, dg_r, dp_s, dp_r, st_sem, own_sem, loc_sem, cb_sem,
):
    p = lax.axis_index("pole")
    b = lax.axis_index("blk")
    x, zl = p // 2, lax.rem(p, 2)
    y, zh, co = b // 4, lax.rem(b // 2, 2), lax.rem(b, 2)
    oz, oc = 1 - zh, 1 - co
    yu, yd, yo = lax.rem(y + 1, 4), lax.rem(y + 3, 4), lax.rem(y + 2, 4)

    def at(yy, zz, cc):
        return yy * 4 + zz * 2 + cc

    up, down, over, sib = (p, at(yu, zh, co)), (p, at(yd, zh, co)), (p, at(y, oz, co)), (p, at(y, zh, oc))

    own = [
        pltpu.make_async_copy(
            l_ref.at[:, k, pl.ds(c * 128, 128)], lbuf.at[c, b, :, pl.ds(k * 128, 128)], own_sem.at[c, k])
        for c in range(CH) for k in range(2)
    ]
    for cp in own:
        cp.start()
    dcopy = pltpu.make_async_copy(d_ref, dv, loc_sem.at[0])
    dcopy.start()

    def g_copy(i):
        return pltpu.make_async_copy(
            g_ref.at[i // 16, :, pl.ds(pl.multiple_of(lax.rem(i, 16) * 256, 256), 256)], stage.at[i], st_sem.at[i])

    def b_copy(i):
        return pltpu.make_async_copy(
            basis_ref.at[pl.ds(pl.multiple_of((i // 4) * 256, 256), 256),
                         pl.ds(pl.multiple_of(lax.rem(i, 4) * 256, 256), 256)], stage.at[i], st_sem.at[i])

    @pl.loop(0, 32)
    def _(i):
        g_copy(i).start()

    bar = pltpu.get_barrier_semaphore()

    @pl.loop(1, 16)
    def _(d):
        pl.semaphore_signal(bar, inc=1, device_id=(p, lax.rem(b + d, 16)), device_id_type=MESH)

    @pl.loop(1, 8)
    def _(d):
        pl.semaphore_signal(bar, inc=1, device_id=(lax.rem(p + d, 8), b), device_id_type=MESH)

    pl.semaphore_wait(bar, 22)
    for cp in own:
        cp.wait()

    def rc(src, dst, s, r, dev):
        return pltpu.make_async_remote_copy(src, dst, s, r, device_id=dev, device_id_type=MESH)

    def ag(c, kind, slot, dev, rows=None):
        ref = lbuf.at[c, slot] if rows is None else lbuf.at[c, slot, pl.ds(rows, 128)]
        return rc(ref, ref, ag_s.at[c, kind], ag_r.at[c, kind], dev)

    def cf(c, i, slot):
        ref = lbuf.at[c, slot]
        return rc(ref, ref, co_s.at[c, i], co_r.at[c, i], sib)

    def slot_of(i, cc):
        return at(lax.rem(y + lax.rem(i, 4), 4), lax.rem(zh + i // 4, 2), cc)

    def own_y(c):
        ag(c, 0, b, up).start()
        ag(c, 1, b, down).start()
        cf(c, 0, b).start()

    def own_z(c):
        ag(c, 2, b, over).start()

    s1, s2, s3, s4 = at(yd, zh, co), at(yu, zh, co), at(y, oz, co), at(yo, zh, co)
    s5, s6, s7 = at(yd, oz, co), at(yu, oz, co), at(yo, oz, co)

    def ring(c):
        ag(c, 0, s1, up).wait_recv()
        ag(c, 3, s1, up, 0).start()
        cf(c, 3, s1).start()
        ag(c, 1, s2, down).wait_recv()
        ag(c, 4, s2, down, 128).start()
        cf(c, 1, s2).start()

    def across(c):
        ag(c, 2, s3, over).wait_recv()
        ag(c, 5, s3, up).start()
        ag(c, 6, s3, down).start()
        cf(c, 4, s3).start()

    def far(c):
        ag(c, 3, s4, up, 0).wait_recv()
        ag(c, 7, s4, over, 0).start()
        ag(c, 4, s4, down, 128).wait_recv()
        ag(c, 8, s4, over, 128).start()
        cf(c, 2, s4).start()

    def late(c):
        ag(c, 5, s5, up).wait_recv()
        cf(c, 7, s5).start()
        ag(c, 6, s6, down).wait_recv()
        cf(c, 5, s6).start()
        ag(c, 7, s7, over, 0).wait_recv()
        ag(c, 8, s7, over, 128).wait_recv()
        cf(c, 6, s7).start()

    def piece(c, slot):
        v = lbuf[c, slot]
        h, l = split(v)
        h2 = jnp.concatenate([-h[:, 128:], h[:, :128]], axis=1)
        l2 = jnp.concatenate([-l[:, 128:], l[:, :128]], axis=1)
        return dot3(gh[slot], gl[slot], h, l) + dot3(gh[16 + slot], gl[16 + slot], h2, l2)

    def products(c, low, high):
        @pl.loop(low, high)
        def _(i):
            acc[...] += piece(c, slot_of(i, co))
            o = slot_of(i, oc)
            cf(c, i, o).wait_recv()
            acc[...] += piece(c, o)

    wr, wi = w_ref[0, 0], w_ref[0, 1]

    def t1(c):
        a = acc[...]
        ar, ai = a[:, :128], a[:, 128:]
        yr, yi = wi * ai - wr * ar, -(wr * ai + wi * ar)
        ybuf[c] = yr
        for d in range(1, 4):
            xx = lax.rem(x + d, 4)
            rc(ybuf.at[c, pl.ds(pl.multiple_of(xx * 64, 64), 64)], rsb.at[c, d], rs_s.at[c, d], rs_r.at[c, d],
               (xx * 2 + zl, b)).start()
        yrh, yrl = split(yr)
        yih, yil = split(yi)
        j = 2 * (c // 2)
        for h in range(2):
            th, tl = lth[j + h], ltl[j + h]
            dpart[c, pl.ds(h * 128, 128)] = dot3(th[:128], tl[:128], yrh, yrl) - dot3(th[128:], tl[128:], yih, yil)

    def t1b(c):
        tot = ybuf[c, pl.ds(pl.multiple_of(x * 64, 64), 64)]
        for d in range(1, 4):
            rc(rsb.at[c, d], rsb.at[c, d], rs_s.at[c, d], rs_r.at[c, d], sib).wait_recv()
            tot = tot + rsb[c, d]
        sb[c] = tot
        rc(sb.at[c], zb.at[c], zl_s.at[c], zl_r.at[c], (x * 2 + 1 - zl, b)).start()

    mine = pl.ds(3 * co, 3)
    theirs = pl.ds(3 * oc, 3)
    others = pl.ds(4 * co, 2)

    def t2(c):
        rc(sb.at[c], zb.at[c], zl_s.at[c], zl_r.at[c], sib).wait_recv()
        mbuf[c, 2 + co, x] = sb[c] + zb[c]
        src = mbuf.at[c, 2 + co, x]
        rc(src, mbuf.at[c, co, x], re_s.at[c, 0], re_r.at[c, co], (p, lax.rem(b + 2 - co, 16))).start()
        rc(src, mbuf.at[c, 4 + co, x], re_s.at[c, 1], re_r.at[c, co], (p, lax.rem(b + 15 - co, 16))).start()
        for d in (2, 1, 3):
            rc(src, src, ao_s.at[c, d], ao_r.at[c, d], (lax.rem(x + d, 4) * 2 + zl, b)).start()

    def sx(c, d, xx, part):
        return rc(mbuf.at[c, part, xx], mbuf.at[c, part, xx], sx_s.at[c, d], sx_r.at[c, d], sib)

    def t3(c):
        for r in range(2):
            got = mbuf.at[c, r + 4 * co, x]
            rc(got, got, re_s.at[c, r], re_r.at[c, r], sib).wait_recv()
        part = mbuf.at[c, others, x]
        for d in (2, 1, 3):
            rc(part, part, ax_s.at[c, d], ax_r.at[c, d], (lax.rem(x + d, 4) * 2 + zl, b)).start()
        sx(c, 0, x, mine).start()

    def t3b(c):
        for d in (1, 3, 2):
            xx = lax.rem(x + 4 - d, 4)
            own_block = mbuf.at[c, 2 + co, xx]
            rc(own_block, own_block, ao_s.at[c, d], ao_r.at[c, d], sib).wait_recv()
            part = mbuf.at[c, others, xx]
            rc(part, part, ax_s.at[c, d], ax_r.at[c, d], sib).wait_recv()
            sx(c, d, xx, mine).start()

    def t4(c):
        for d in (0, 1, 3, 2):
            sx(c, d, lax.rem(x + 4 - d, 4), theirs).wait_recv()
        for k in range(6):
            for q in range(4):
                mloc[k * 4 + q] = mbuf[c, k, q]
        count = cnt_ref[0]
        first = (b - co - REACH) * 2

        @pl.loop(0, 8)
        def _(s):
            n = jnp.clip(ids_ref[0, s] - first, 0, 11)
            keep = jnp.where(s < count, 1.0, 0.0).astype(F32)
            for i in range(2):
                h, l = split(mloc[n * 2 + i] * keep)
                rows = pl.ds(pl.multiple_of(s * 128 + i * 64, 64), 64)
                selh[rows, :128] = h
                selh[rows, 128:] = l

        @pl.loop(0, 4)
        def _(r):
            pq = dot(bh[r], selh[...])
            q = dot(bl[r], selh[:, :128])
            rows = pl.ds(pl.multiple_of(r * 512, 512), 512)
            dacc[rows] += (pq[:, :128] + pq[:, 128:] + q) * cbuf[c, rows]

    def begin(c):
        acc[...] = jnp.zeros_like(acc)
        products(c, 0, 5)

    def finish(c):
        products(c, 5, 8)
        t1(c)

    steps = {"Y": own_y, "V": own_z, "E": ring, "Z": across, "F": far, "H": late, "P": begin, "Q": finish,
             "1": t1b, "2": t2, "3": t3, "B": t3b, "4": t4}

    own_y(0)
    own_z(0)
    own_y(1)
    own_z(1)

    @pl.loop(0, 32)
    def _(i):
        g_copy(i).wait()
        h, l = split(stage[i])
        gh[i] = h
        gl[i] = l
        b_copy(i).start()

    for c in range(CH):
        pltpu.make_async_copy(cb_ref.at[:, pl.ds(c * 128, 128)], cbuf.at[c], cb_sem.at[c]).start()

    @pl.loop(0, CH)
    def _(c):
        h, l = split(lbuf[c, b].T)
        lth[c] = h
        ltl[c] = l

    def basis_split(_):
        @pl.loop(0, 32)
        def _(i):
            b_copy(i).wait()
            h, l = split(stage[i])
            bh[i // 8, pl.ds(pl.multiple_of(lax.rem(i // 4, 2) * 256, 256), 256), pl.ds(pl.multiple_of(lax.rem(i, 4) * 256, 256), 256)] = h
            bl[i // 8, pl.ds(pl.multiple_of(lax.rem(i // 4, 2) * 256, 256), 256), pl.ds(pl.multiple_of(lax.rem(i, 4) * 256, 256), 256)] = l

        for c in range(CH):
            pltpu.make_async_copy(cb_ref.at[:, pl.ds(c * 128, 128)], cbuf.at[c], cb_sem.at[c]).wait()
        dcopy.wait()
        dacc[...] = jnp.zeros_like(dacc)

    def dg(d, row):
        return rc(dpart.at[:, pl.ds(pl.multiple_of(row * 16, 16), 16)], dgb.at[d], dg_s.at[d], dg_r.at[d],
                  (p, lax.rem(b + d, 16)))

    def dp(d):
        return rc(dsum, dpb.at[d], dp_s.at[d], dp_r.at[d], (lax.rem(p + d, 8), b))

    def diag_send(_):
        @pl.loop(1, 16)
        def _(d):
            dg(d, lax.rem(b + d, 16)).start()

    def diag_sum(_):
        dsum[...] = dpart[:, pl.ds(pl.multiple_of(b * 16, 16), 16)]

        @pl.loop(1, 16)
        def _(d):
            dg(d, 0).wait_recv()
            dsum[...] += dgb[d]

        for c in range(CH):
            cols = slice((c % 2) * 128, (c % 2) * 128 + 128)
            dsum[c] = wr * dv[0, c // 2, :, cols] - wi * dv[1, c // 2, :, cols] - dsum[c]

        @pl.loop(1, 8)
        def _(d):
            dp(d).start()

    steps.update({"C": basis_split, "D": diag_send, "S": diag_sum})

    for ev, c in events():
        steps[ev](c)

    for r in range(16):
        dens_ref[r, :] = jnp.sum(dacc[r * 128 : (r + 1) * 128].T, axis=0)

    dpb[0] = dsum[...]

    @pl.loop(1, 8)
    def _(d):
        dp(d).wait_recv()
        dpb[0] += dpb[d]

    for c in range(CH):
        diag_ref[c // 2, :, (c % 2) * 128 : (c % 2) * 128 + 128] = dpb[0, c]

    @pl.loop(0, CH)
    def _(c):
        for kind in range(9):
            rows = {3: 0, 4: 128, 7: 0, 8: 128}.get(kind)
            ag(c, kind, b, sib, rows).wait_send()
        for i in range(8):
            cf(c, i, b).wait_send()
        for d in range(1, 4):
            rc(rsb.at[c, d], rsb.at[c, d], rs_s.at[c, d], rs_r.at[c, d], sib).wait_send()
            rc(mbuf.at[c, others, x], mbuf.at[c, others, x], ax_s.at[c, d], ax_r.at[c, d], sib).wait_send()
            rc(mbuf.at[c, 2 + co, x], mbuf.at[c, 2 + co, x], ao_s.at[c, d], ao_r.at[c, d], sib).wait_send()
        rc(sb.at[c], zb.at[c], zl_s.at[c], zl_r.at[c], sib).wait_send()
        for k in range(2):
            rc(mbuf.at[c, k, x], mbuf.at[c, k, x], re_s.at[c, k], re_r.at[c, k], sib).wait_send()
        for d in range(4):
            sx(c, d, x, mine).wait_send()

    @pl.loop(1, 16)
    def _(d):
        dg(d, 0).wait_send()

    @pl.loop(1, 8)
    def _(d):
        dp(d).wait_send()


def body(inverse_block, factor, diag_inverse, pole_weight, block_ids, block_count, basis, column_basis):
    dma = pltpu.SemaphoreType.DMA
    anyspace = pl.BlockSpec(memory_space=pl.ANY)
    smem = pl.BlockSpec(memory_space=pltpu.SMEM)
    vmem = pl.BlockSpec(memory_space=pltpu.VMEM)
    diag, dens = pl.pallas_call(
        kernel,
        name="selinv",
        out_shape=(jax.ShapeDtypeStruct((2, 16, 256), F32), jax.ShapeDtypeStruct((16, 128), F32)),
        in_specs=[smem, smem, smem, anyspace, anyspace, anyspace, anyspace, anyspace],
        out_specs=(vmem, vmem),
        scratch_shapes=[
            pltpu.VMEM((CH, 16, 256, 256), F32),
            pltpu.VMEM((32, 256, 256), BF16),
            pltpu.VMEM((32, 256, 256), BF16),
            pltpu.VMEM((32, 256, 256), F32),
            pltpu.VMEM((4, 512, 1024), BF16),
            pltpu.VMEM((4, 512, 1024), BF16),
            pltpu.VMEM((CH, 2048, 128), F32),
            pltpu.VMEM((CH, 6, 4, 64, 128), F32),
            pltpu.VMEM((CH, 256, 128), F32),
            pltpu.VMEM((CH, 4, 64, 128), F32),
            pltpu.VMEM((CH, 64, 128), F32),
            pltpu.VMEM((CH, 64, 128), F32),
            pltpu.VMEM((CH, 256, 128), F32),
            pltpu.VMEM((16, CH, 16, 128), F32),
            pltpu.VMEM((8, CH, 16, 128), F32),
            pltpu.VMEM((CH, 16, 128), F32),
            pltpu.VMEM((256, 256), F32),
            pltpu.VMEM((2048, 128), F32),
            pltpu.VMEM((1024, 256), BF16),
            pltpu.VMEM((CH, 256, 256), BF16),
            pltpu.VMEM((CH, 256, 256), BF16),
            pltpu.VMEM((2, 2, 16, 256), F32),
            pltpu.VMEM((24, 64, 128), F32),
            dma((CH, 9)), dma((CH, 9)), dma((CH, 8)), dma((CH, 8)),
            dma((CH, 4)), dma((CH, 4)), dma((CH,)), dma((CH,)), dma((CH, 2)), dma((CH, 2)), dma((CH, 4)), dma((CH, 4)), dma((CH, 4)), dma((CH, 4)), dma((CH, 4)), dma((CH, 4)),
            dma((16,)), dma((16,)), dma((8,)), dma((8,)), dma((32,)), dma((CH, 2)), dma((1,)), dma((CH,)),
        ],
        compiler_params=pltpu.CompilerParams(
            collective_id=0, has_side_effects=True, vmem_limit_bytes=67_000_000),
    )(pole_weight, block_ids, block_count,
      inverse_block[0], factor[0], diag_inverse[0], basis[0], column_basis[0])
    return diag, dens.reshape(1, 2048)


def solution(mesh):
    in_specs = (
        P("pole", None, "blk", None),
        P("pole", "blk", None, None),
        P("pole", None, None, "blk", None),
        P("pole", None),
        P(("pole", "blk"), None),
        P(("pole", "blk")),
        P(("pole", "blk"), None, None),
        P(("pole", "blk"), None, None),
    )
    out_specs = (P(None, "blk", None), P(("pole", "blk"), None))
    return jax.shard_map(body, mesh=mesh, in_specs=in_specs, out_specs=out_specs, check_vma=False)
```

```python
import jax
import jax.numpy as jnp
from jax import lax
from jax.experimental import pallas as pl
from jax.experimental.pallas import tpu as pltpu
from jax.sharding import PartitionSpec as P

MESH = pl.DeviceIdType.MESH
F32 = jnp.float32
BF16 = jnp.bfloat16
CH = 4
REACH = 2


ORDER = (
    "E0Z0C0Y2V2E1Z1F0",
    "P0Y3H0Q0V3F1E2P1",
    "10H1Q1E3Z2F2Z3P2",
    "2011H2Q230F3P3H3",
    "Q31221132231B023",
    "403233B1D041B242",
    "B3S043",
)


def events():
    text = "".join(ORDER)
    return [(text[i], int(text[i + 1])) for i in range(0, len(text), 2)]


def split(x):
    high = x.astype(BF16)
    return high, (x - high.astype(F32)).astype(BF16)


def dot(a, b):
    return jnp.dot(a, b, preferred_element_type=F32)


def dot3(ah, al, bh, bl):
    return dot(ah, bh) + dot(ah, bl) + dot(al, bh)


def kernel(
    w_ref, ids_ref, cnt_ref, g_ref, l_ref, d_ref, basis_ref, cb_ref,
    diag_ref, dens_ref,
    lbuf, gh, gl, stage, bh, bl, cbuf, mbuf, ybuf, rsb, sb, zb, dpart, dgb, dpb, dsum,
    acc, dacc, selh, lth, ltl, dv, mloc,
    ag_s, ag_r, co_s, co_r, rs_s, rs_r, zl_s, zl_r, re_s, re_r, ao_s, ao_r, ax_s, ax_r, sx_s, sx_r,
    dg_s, dg_r, dp_s, dp_r, st_sem, own_sem, loc_sem, cb_sem,
):
    p = lax.axis_index("pole")
    b = lax.axis_index("blk")
    x, zl = p // 2, lax.rem(p, 2)
    y, zh, co = b // 4, lax.rem(b // 2, 2), lax.rem(b, 2)
    oz, oc = 1 - zh, 1 - co
    yu, yd, yo = lax.rem(y + 1, 4), lax.rem(y + 3, 4), lax.rem(y + 2, 4)

    def at(yy, zz, cc):
        return yy * 4 + zz * 2 + cc

    up, down, over, sib = (p, at(yu, zh, co)), (p, at(yd, zh, co)), (p, at(y, oz, co)), (p, at(y, zh, oc))

    own = [
        pltpu.make_async_copy(
            l_ref.at[:, k, pl.ds(c * 128, 128)], lbuf.at[c, b, :, pl.ds(k * 128, 128)], own_sem.at[c, k])
        for c in range(CH) for k in range(2)
    ]
    for cp in own:
        cp.start()
    dcopy = pltpu.make_async_copy(d_ref, dv, loc_sem.at[0])
    dcopy.start()

    def g_copy(i):
        return pltpu.make_async_copy(
            g_ref.at[i // 16, :, pl.ds(pl.multiple_of(lax.rem(i, 16) * 256, 256), 256)], stage.at[i], st_sem.at[i])

    def b_copy(i):
        return pltpu.make_async_copy(
            basis_ref.at[pl.ds(pl.multiple_of((i // 4) * 256, 256), 256),
                         pl.ds(pl.multiple_of(lax.rem(i, 4) * 256, 256), 256)], stage.at[i], st_sem.at[i])

    @pl.loop(0, 32)
    def _(i):
        g_copy(i).start()

    bar = pltpu.get_barrier_semaphore()

    @pl.loop(1, 16)
    def _(d):
        pl.semaphore_signal(bar, inc=1, device_id=(p, lax.rem(b + d, 16)), device_id_type=MESH)

    @pl.loop(1, 8)
    def _(d):
        pl.semaphore_signal(bar, inc=1, device_id=(lax.rem(p + d, 8), b), device_id_type=MESH)

    pl.semaphore_wait(bar, 22)
    for cp in own:
        cp.wait()

    def rc(src, dst, s, r, dev):
        return pltpu.make_async_remote_copy(src, dst, s, r, device_id=dev, device_id_type=MESH)

    def ag(c, kind, slot, dev, rows=None):
        ref = lbuf.at[c, slot] if rows is None else lbuf.at[c, slot, pl.ds(rows, 128)]
        return rc(ref, ref, ag_s.at[c, kind], ag_r.at[c, kind], dev)

    def cf(c, i, slot):
        ref = lbuf.at[c, slot]
        return rc(ref, ref, co_s.at[c, i], co_r.at[c, i], sib)

    def slot_of(i, cc):
        return at(lax.rem(y + lax.rem(i, 4), 4), lax.rem(zh + i // 4, 2), cc)

    def own_y(c):
        ag(c, 0, b, up).start()
        ag(c, 1, b, down).start()
        cf(c, 0, b).start()

    def own_z(c):
        ag(c, 2, b, over).start()

    s1, s2, s3, s4 = at(yd, zh, co), at(yu, zh, co), at(y, oz, co), at(yo, zh, co)
    s5, s6, s7 = at(yd, oz, co), at(yu, oz, co), at(yo, oz, co)

    def ring(c):
        ag(c, 0, s1, up).wait_recv()
        ag(c, 3, s1, up, 0).start()
        cf(c, 3, s1).start()
        ag(c, 1, s2, down).wait_recv()
        ag(c, 4, s2, down, 128).start()
        cf(c, 1, s2).start()

    def across(c):
        ag(c, 2, s3, over).wait_recv()
        ag(c, 5, s3, up).start()
        ag(c, 6, s3, down).start()
        cf(c, 4, s3).start()

    def far(c):
        ag(c, 3, s4, up, 0).wait_recv()
        ag(c, 7, s4, over, 0).start()
        ag(c, 4, s4, down, 128).wait_recv()
        ag(c, 8, s4, over, 128).start()
        cf(c, 2, s4).start()

    def late(c):
        ag(c, 5, s5, up).wait_recv()
        cf(c, 7, s5).start()
        ag(c, 6, s6, down).wait_recv()
        cf(c, 5, s6).start()
        ag(c, 7, s7, over, 0).wait_recv()
        ag(c, 8, s7, over, 128).wait_recv()
        cf(c, 6, s7).start()

    def piece(c, slot):
        v = lbuf[c, slot]
        h, l = split(v)
        h2 = jnp.concatenate([-h[:, 128:], h[:, :128]], axis=1)
        l2 = jnp.concatenate([-l[:, 128:], l[:, :128]], axis=1)
        return dot3(gh[slot], gl[slot], h, l) + dot3(gh[16 + slot], gl[16 + slot], h2, l2)

    def products(c, low, high):
        @pl.loop(low, high)
        def _(i):
            acc[...] += piece(c, slot_of(i, co))
            o = slot_of(i, oc)
            cf(c, i, o).wait_recv()
            acc[...] += piece(c, o)

    wr, wi = w_ref[0, 0], w_ref[0, 1]

    def t1(c):
        a = acc[...]
        ar, ai = a[:, :128], a[:, 128:]
        yr, yi = wi * ai - wr * ar, -(wr * ai + wi * ar)
        ybuf[c] = yr
        for d in range(1, 4):
            xx = lax.rem(x + d, 4)
            rc(ybuf.at[c, pl.ds(pl.multiple_of(xx * 64, 64), 64)], rsb.at[c, d], rs_s.at[c, d], rs_r.at[c, d],
               (xx * 2 + zl, b)).start()
        yrh, yrl = split(yr)
        yih, yil = split(yi)
        j = 2 * (c // 2)
        for h in range(2):
            th, tl = lth[j + h], ltl[j + h]
            dpart[c, pl.ds(h * 128, 128)] = dot3(th[:128], tl[:128], yrh, yrl) - dot3(th[128:], tl[128:], yih, yil)

    def t1b(c):
        tot = ybuf[c, pl.ds(pl.multiple_of(x * 64, 64), 64)]
        for d in range(1, 4):
            rc(rsb.at[c, d], rsb.at[c, d], rs_s.at[c, d], rs_r.at[c, d], sib).wait_recv()
            tot = tot + rsb[c, d]
        sb[c] = tot
        rc(sb.at[c], zb.at[c], zl_s.at[c], zl_r.at[c], (x * 2 + 1 - zl, b)).start()

    mine = pl.ds(3 * co, 3)
    theirs = pl.ds(3 * oc, 3)
    others = pl.ds(4 * co, 2)

    def t2(c):
        rc(sb.at[c], zb.at[c], zl_s.at[c], zl_r.at[c], sib).wait_recv()
        mbuf[c, 2 + co, x] = sb[c] + zb[c]
        src = mbuf.at[c, 2 + co, x]
        rc(src, mbuf.at[c, co, x], re_s.at[c, 0], re_r.at[c, co], (p, lax.rem(b + 2 - co, 16))).start()
        rc(src, mbuf.at[c, 4 + co, x], re_s.at[c, 1], re_r.at[c, co], (p, lax.rem(b + 15 - co, 16))).start()
        for d in (2, 1, 3):
            rc(src, src, ao_s.at[c, d], ao_r.at[c, d], (lax.rem(x + d, 4) * 2 + zl, b)).start()

    def sx(c, d, xx, part):
        return rc(mbuf.at[c, part, xx], mbuf.at[c, part, xx], sx_s.at[c, d], sx_r.at[c, d], sib)

    def t3(c):
        for r in range(2):
            got = mbuf.at[c, r + 4 * co, x]
            rc(got, got, re_s.at[c, r], re_r.at[c, r], sib).wait_recv()
        part = mbuf.at[c, others, x]
        for d in (2, 1, 3):
            rc(part, part, ax_s.at[c, d], ax_r.at[c, d], (lax.rem(x + d, 4) * 2 + zl, b)).start()
        sx(c, 0, x, mine).start()

    def t3b(c):
        for d in (1, 3, 2):
            xx = lax.rem(x + 4 - d, 4)
            own_block = mbuf.at[c, 2 + co, xx]
            rc(own_block, own_block, ao_s.at[c, d], ao_r.at[c, d], sib).wait_recv()
            part = mbuf.at[c, others, xx]
            rc(part, part, ax_s.at[c, d], ax_r.at[c, d], sib).wait_recv()
            sx(c, d, xx, mine).start()

    def t4(c):
        for d in (0, 1, 3, 2):
            sx(c, d, lax.rem(x + 4 - d, 4), theirs).wait_recv()
        for k in range(6):
            for q in range(4):
                mloc[k * 4 + q] = mbuf[c, k, q]
        count = cnt_ref[0]
        first = (b - co - REACH) * 2

        @pl.loop(0, 8)
        def _(s):
            n = jnp.clip(ids_ref[0, s] - first, 0, 11)
            keep = jnp.where(s < count, 1.0, 0.0).astype(F32)
            for i in range(2):
                h, l = split(mloc[n * 2 + i] * keep)
                rows = pl.ds(pl.multiple_of(s * 128 + i * 64, 64), 64)
                selh[rows, :128] = h
                selh[rows, 128:] = l

        @pl.loop(0, 4)
        def _(r):
            pq = dot(bh[r], selh[...])
            q = dot(bl[r], selh[:, :128])
            rows = pl.ds(pl.multiple_of(r * 512, 512), 512)
            dacc[rows] += (pq[:, :128] + pq[:, 128:] + q) * cbuf[c, rows]

    def begin(c):
        acc[...] = jnp.zeros_like(acc)
        products(c, 0, 5)

    def finish(c):
        products(c, 5, 8)
        t1(c)

    steps = {"Y": own_y, "V": own_z, "E": ring, "Z": across, "F": far, "H": late, "P": begin, "Q": finish,
             "1": t1b, "2": t2, "3": t3, "B": t3b, "4": t4}

    own_y(0)
    own_z(0)
    own_y(1)
    own_z(1)

    @pl.loop(0, 32)
    def _(i):
        g_copy(i).wait()
        h, l = split(stage[i])
        gh[i] = h
        gl[i] = l
        b_copy(i).start()

    for c in range(CH):
        pltpu.make_async_copy(cb_ref.at[:, pl.ds(c * 128, 128)], cbuf.at[c], cb_sem.at[c]).start()

    @pl.loop(0, CH)
    def _(c):
        h, l = split(lbuf[c, b].T)
        lth[c] = h
        ltl[c] = l

    def basis_split(_):
        @pl.loop(0, 32)
        def _(i):
            b_copy(i).wait()
            h, l = split(stage[i])
            bh[i // 8, pl.ds(pl.multiple_of(lax.rem(i // 4, 2) * 256, 256), 256), pl.ds(pl.multiple_of(lax.rem(i, 4) * 256, 256), 256)] = h
            bl[i // 8, pl.ds(pl.multiple_of(lax.rem(i // 4, 2) * 256, 256), 256), pl.ds(pl.multiple_of(lax.rem(i, 4) * 256, 256), 256)] = l

        for c in range(CH):
            pltpu.make_async_copy(cb_ref.at[:, pl.ds(c * 128, 128)], cbuf.at[c], cb_sem.at[c]).wait()
        dcopy.wait()
        dacc[...] = jnp.zeros_like(dacc)

    def dg(d, row):
        return rc(dpart.at[:, pl.ds(pl.multiple_of(row * 16, 16), 16)], dgb.at[d], dg_s.at[d], dg_r.at[d],
                  (p, lax.rem(b + d, 16)))

    def dp(d):
        return rc(dsum, dpb.at[d], dp_s.at[d], dp_r.at[d], (lax.rem(p + d, 8), b))

    def diag_send(_):
        @pl.loop(1, 16)
        def _(d):
            dg(d, lax.rem(b + d, 16)).start()

    def diag_sum(_):
        dsum[...] = dpart[:, pl.ds(pl.multiple_of(b * 16, 16), 16)]

        @pl.loop(1, 16)
        def _(d):
            dg(d, 0).wait_recv()
            dsum[...] += dgb[d]

        for c in range(CH):
            cols = slice((c % 2) * 128, (c % 2) * 128 + 128)
            dsum[c] = wr * dv[0, c // 2, :, cols] - wi * dv[1, c // 2, :, cols] - dsum[c]

        @pl.loop(1, 8)
        def _(d):
            dp(d).start()

    steps.update({"C": basis_split, "D": diag_send, "S": diag_sum})

    for ev, c in events():
        steps[ev](c)

    for r in range(16):
        dens_ref[r, :] = jnp.sum(dacc[r * 128 : (r + 1) * 128].T, axis=0)

    dpb[0] = dsum[...]

    @pl.loop(1, 8)
    def _(d):
        dp(d).wait_recv()
        dpb[0] += dpb[d]

    for c in range(CH):
        diag_ref[c // 2, :, (c % 2) * 128 : (c % 2) * 128 + 128] = dpb[0, c]

    @pl.loop(0, CH)
    def _(c):
        for kind in range(9):
            rows = {3: 0, 4: 128, 7: 0, 8: 128}.get(kind)
            ag(c, kind, b, sib, rows).wait_send()
        for i in range(8):
            cf(c, i, b).wait_send()
        for d in range(1, 4):
            rc(rsb.at[c, d], rsb.at[c, d], rs_s.at[c, d], rs_r.at[c, d], sib).wait_send()
            rc(mbuf.at[c, others, x], mbuf.at[c, others, x], ax_s.at[c, d], ax_r.at[c, d], sib).wait_send()
            rc(mbuf.at[c, 2 + co, x], mbuf.at[c, 2 + co, x], ao_s.at[c, d], ao_r.at[c, d], sib).wait_send()
        rc(sb.at[c], zb.at[c], zl_s.at[c], zl_r.at[c], sib).wait_send()
        for k in range(2):
            rc(mbuf.at[c, k, x], mbuf.at[c, k, x], re_s.at[c, k], re_r.at[c, k], sib).wait_send()
        for d in range(4):
            sx(c, d, x, mine).wait_send()

    @pl.loop(1, 16)
    def _(d):
        dg(d, 0).wait_send()

    @pl.loop(1, 8)
    def _(d):
        dp(d).wait_send()


def body(inverse_block, factor, diag_inverse, pole_weight, block_ids, block_count, basis, column_basis):
    dma = pltpu.SemaphoreType.DMA
    anyspace = pl.BlockSpec(memory_space=pl.ANY)
    smem = pl.BlockSpec(memory_space=pltpu.SMEM)
    vmem = pl.BlockSpec(memory_space=pltpu.VMEM)
    diag, dens = pl.pallas_call(
        kernel,
        name="selinv",
        out_shape=(jax.ShapeDtypeStruct((2, 16, 256), F32), jax.ShapeDtypeStruct((16, 128), F32)),
        in_specs=[smem, smem, smem, anyspace, anyspace, anyspace, anyspace, anyspace],
        out_specs=(vmem, vmem),
        scratch_shapes=[
            pltpu.VMEM((CH, 16, 256, 256), F32),
            pltpu.VMEM((32, 256, 256), BF16),
            pltpu.VMEM((32, 256, 256), BF16),
            pltpu.VMEM((32, 256, 256), F32),
            pltpu.VMEM((4, 512, 1024), BF16),
            pltpu.VMEM((4, 512, 1024), BF16),
            pltpu.VMEM((CH, 2048, 128), F32),
            pltpu.VMEM((CH, 6, 4, 64, 128), F32),
            pltpu.VMEM((CH, 256, 128), F32),
            pltpu.VMEM((CH, 4, 64, 128), F32),
            pltpu.VMEM((CH, 64, 128), F32),
            pltpu.VMEM((CH, 64, 128), F32),
            pltpu.VMEM((CH, 256, 128), F32),
            pltpu.VMEM((16, CH, 16, 128), F32),
            pltpu.VMEM((8, CH, 16, 128), F32),
            pltpu.VMEM((CH, 16, 128), F32),
            pltpu.VMEM((256, 256), F32),
            pltpu.VMEM((2048, 128), F32),
            pltpu.VMEM((1024, 256), BF16),
            pltpu.VMEM((CH, 256, 256), BF16),
            pltpu.VMEM((CH, 256, 256), BF16),
            pltpu.VMEM((2, 2, 16, 256), F32),
            pltpu.VMEM((24, 64, 128), F32),
            dma((CH, 9)), dma((CH, 9)), dma((CH, 8)), dma((CH, 8)),
            dma((CH, 4)), dma((CH, 4)), dma((CH,)), dma((CH,)), dma((CH, 2)), dma((CH, 2)), dma((CH, 4)), dma((CH, 4)), dma((CH, 4)), dma((CH, 4)), dma((CH, 4)), dma((CH, 4)),
            dma((16,)), dma((16,)), dma((8,)), dma((8,)), dma((32,)), dma((CH, 2)), dma((1,)), dma((CH,)),
        ],
        compiler_params=pltpu.CompilerParams(
            collective_id=0, has_side_effects=True, vmem_limit_bytes=67_000_000),
    )(pole_weight, block_ids, block_count,
      inverse_block[0], factor[0], diag_inverse[0], basis[0], column_basis[0])
    return diag, dens.reshape(1, 2048)


def solution(mesh):
    in_specs = (
        P("pole", None, "blk", None),
        P("pole", "blk", None, None),
        P("pole", None, None, "blk", None),
        P("pole", None),
        P(("pole", "blk"), None),
        P(("pole", "blk")),
        P(("pole", "blk"), None, None),
        P(("pole", "blk"), None, None),
    )
    out_specs = (P(None, "blk", None), P(("pole", "blk"), None))
    return jax.shard_map(body, mesh=mesh, in_specs=in_specs, out_specs=out_specs, check_vma=False)
```
